32 devices in a mesh: grp: 2 (over x), exp: 16 (over z, y, core).
Axes of the slice: x: 2, y: 2, z: 4, core: 2. Of those that a mesh axis runs over, the one named last changes fastest.
Arguments:
- tokens: bfloat16 [192, 196, 768], P(('grp', 'exp')), parts along dimension 0, may hold values from -6 to 6
- logits: float32 [192, 196, 16], P(('grp', 'exp')), parts along dimension 0, may hold values from -8 to 400
- slot_out: bfloat16 [32, 96, 768], P(('grp', 'exp')), parts along dimension 0, may hold values from -1.5 to 1.5
- slot_in: bfloat16 [32, 96, 768], P(('grp', 'exp')), parts along dimension 0, may hold values from -6 to 6
- out_grad: bfloat16 [192, 196, 768], P(('grp', 'exp')), parts along dimension 0, may hold values from -192 to 192
- router: bfloat16 [16, 768], replicated, may hold values from -0.21875 to 0.21875
- w_in: bfloat16 [16, 768, 3072], P('exp'), may hold values from -0.21875 to 0.21875
- bias_in: float32 [16, 3072], P('exp'), may hold values from -5 to 5
- w_out: bfloat16 [16, 3072, 768], P('exp'), may hold values from -0.109375 to 0.109375
Outputs:
- input_grad: bfloat16 [192, 196, 768], P(('grp', 'exp')), parts along dimension 0
- router_grad: float32 [32, 768], P(('grp', 'exp')), parts along dimension 0
The draws below stay inside these ranges and needn't reach their ends.
There are 2 independent parts, one for each index of `grp`. The reference program is written for one: setup_inputs(seed, part) draws one part's arguments, and reference() takes and returns one part's arrays. A program takes and returns all parts, laid end to end along the dimension named above; an argument that names none is the same for every part. Nothing has to cross between parts.
All inputs are finite; a program needn't handle non-finite values.
Results may differ from the reference program's by a relative error of at most 0.0075.
Values may be sent and summed in bfloat16 or wider, within the bound.
A program may use at most 64 MiB of HBM per device.

```python
import jax
import jax.numpy as jnp
from jax import lax

D = 768
FF = 3072
SEQ = 196
EXPERTS = 16
IMAGES = 96


def draw_logits(key, part):
    base = jnp.clip(1.5 * jax.random.normal(key, (IMAGES, SEQ, EXPERTS), jnp.float32), -6.0, 6.0)
    return base


def steps_of(stream_key, dims, shards, least, high):
    def one(axis_at, parts):
        steps = jax.random.uniform(jax.random.fold_in(jax.random.fold_in(stream_key, 6), axis_at), (parts,), jnp.float32, least / len(shards), high / len(shards))
        return jnp.repeat(jnp.exp(steps), dims[axis_at] // parts).reshape((-1,) + (1,) * (len(dims) - axis_at - 1))

    loudness = one(*shards[0])
    for cut in shards[1:]:
        loudness = loudness * one(*cut)
    return loudness


def noise(stream_key, extent, width, most, shards=(), dtype=jnp.bfloat16):
    result = jax.random.normal(stream_key, extent, jnp.float32) * width
    if len(shards) > 0:
        result = steps_of(stream_key, extent, shards, -0.22, 0.18) * result
    return jnp.clip(result, min=-most, max=most).astype(dtype)


def setup_inputs(seed: int = 0, part: int = 0) -> dict:
    key_of = jax.random.split(jax.random.key(seed), 10)
    own_keys = jax.random.split(jax.random.fold_in(key_of[9], part), 10)
    tokens = noise(own_keys[0], (IMAGES, SEQ, D), 1.0, 6.0, ((0, 16),))
    logits = draw_logits(jax.random.fold_in(jax.random.fold_in(key_of[9], part), 71), part)
    slot_out = noise(own_keys[2], (EXPERTS, IMAGES, D), 0.25, 1.5, ((0, 16),))
    slot_in = noise(own_keys[3], (EXPERTS, IMAGES, D), 1.0, 6.0, ((0, 16),))
    out_grad = noise(own_keys[4], (IMAGES, SEQ, D), 32.0, 192.0, ((0, 16),))
    router = noise(key_of[5], (EXPERTS, D), D ** -0.5, 0.21875)
    w_in = noise(key_of[6], (EXPERTS, D, FF), D ** -0.5, 0.21875, ((0, 16),))
    bias_in = noise(key_of[7], (EXPERTS, FF), 1.0, 5.0, ((0, 16),), jnp.float32)
    w_out = noise(key_of[8], (EXPERTS, FF, D), FF ** -0.5, 0.109375, ((0, 16),))
    return dict(tokens=tokens, logits=logits, slot_out=slot_out, slot_in=slot_in, out_grad=out_grad, router=router, w_in=w_in, bias_in=bias_in, w_out=w_out)


gelu_root = 0.7978845608028654
gelu_cubic = 0.044715


def gelu_slope(values):
    inner_arg = gelu_root * (values + gelu_cubic * values * values * values)
    tanh_val = jnp.tanh(inner_arg)
    return 0.5 * (1.0 + tanh_val) + 0.5 * values * (1.0 - tanh_val * tanh_val) * gelu_root * (1.0 + 3.0 * gelu_cubic * values * values)


def expert_backward(inputs):
    slot_rows, slot_grads, weight_in, bias_row, weight_out = inputs
    hidden_pre = jnp.dot(slot_rows, weight_in, preferred_element_type=jnp.float32) + bias_row
    hidden_grad = jnp.dot(slot_grads, weight_out.T, preferred_element_type=jnp.float32)
    pre_grad = (hidden_grad * gelu_slope(hidden_pre)).astype(jnp.bfloat16)
    return jnp.dot(pre_grad, weight_in.T, preferred_element_type=jnp.float32).astype(jnp.bfloat16)


def reference(tokens, logits, slot_out, slot_in, out_grad, router, w_in, bias_in, w_out):
    dispatch = jax.nn.softmax(logits, axis=1)
    combine = jax.nn.softmax(logits, axis=2)
    combine_rounded = combine.astype(jnp.bfloat16)
    dispatch_rounded = dispatch.astype(jnp.bfloat16)
    tokens_wide = tokens.astype(jnp.float32)
    grad_wide = out_grad.astype(jnp.float32)
    slot_grad = jnp.einsum("itj,itd->jid", combine_rounded.astype(jnp.float32), grad_wide).astype(jnp.bfloat16)
    slot_in_grad = lax.map(expert_backward, (slot_in, slot_grad, w_in, bias_in, w_out))
    in_grad_wide = slot_in_grad.astype(jnp.float32)
    combine_grad = jnp.einsum("itd,jid->itj", grad_wide, slot_out.astype(jnp.float32))
    comb_logit = (combine * (combine_grad - jnp.sum(combine * combine_grad, axis=2, keepdims=True))).astype(jnp.bfloat16)
    dispatch_grad = jnp.einsum("itd,jid->itj", tokens_wide, in_grad_wide)
    disp_logit = (dispatch * (dispatch_grad - jnp.sum(dispatch * dispatch_grad, axis=1, keepdims=True))).astype(jnp.bfloat16)
    router_wide = router.astype(jnp.float32)
    comb_wide = comb_logit.astype(jnp.float32)
    disp_wide = disp_logit.astype(jnp.float32)
    input_grad = jnp.einsum("itj,jid->itd", dispatch_rounded.astype(jnp.float32), in_grad_wide)
    input_grad = input_grad + jnp.einsum("itj,jd->itd", comb_wide, router_wide)
    input_grad = input_grad + jnp.einsum("itj,jd->itd", disp_wide, router_wide)
    router_grad = jnp.einsum("itj,itd->jd", comb_wide, tokens_wide) + jnp.einsum("itj,itd->jd", disp_wide, tokens_wide)
    router_grad = router_grad / IMAGES
    return input_grad.astype(jnp.bfloat16), router_grad
```

```python
import functools

import jax
import jax.numpy as jnp
from jax import lax
from jax.experimental import pallas as pl
from jax.experimental.pallas import tpu as pltpu
from jax.sharding import PartitionSpec as P

gelu_root = 0.7978845608028654
gelu_cubic = 0.044715
MESH = pl.DeviceIdType.MESH
F32 = jnp.float32
BF16 = jnp.bfloat16


def gelu_slope(values):
    square = values * values
    inner_arg = gelu_root * (values + gelu_cubic * square * values)
    tanh_val = jnp.tanh(inner_arg)
    return 0.5 * (1.0 + tanh_val) + 0.5 * values * (1.0 - tanh_val * tanh_val) * gelu_root * (
        1.0 + 3.0 * gelu_cubic * square
    )


def dot(a, b):
    return lax.dot_general(a, b, (((1,), (0,)), ((), ())), preferred_element_type=F32)


def dot_nt(a, b):
    return lax.dot_general(a, b, (((1,), (1,)), ((), ())), preferred_element_type=F32)


def dot_tn(a, b):
    return lax.dot_general(a, b, (((0,), (0,)), ((), ())), preferred_element_type=F32)


def ones_where(rows, cols, wanted):
    r = lax.broadcasted_iota(jnp.int32, (rows, cols), 0)
    c = lax.broadcasted_iota(jnp.int32, (rows, cols), 1)
    return jnp.where(wanted(r, c), 1.0, 0.0).astype(BF16)


def body(
    n, b, pad, chunk,
    tok_hbm, log_hbm, so_hbm, si_hbm, og_hbm, rt_hbm, wi_hbm, bi_hbm, wo_hbm,
    ig_hbm, rg_ref,
    tok, logv, so, si, og, rt, wi, bi, wo, igv,
    comb, disp, combl, displ, slope, sg, sip,
    send_s, recv_s, send_a, recv_a, send_b, recv_b, send_r, recv_r,
    load_sem, out_sem, ss, rs, sa, ra, sb, rb, sr, rr,
):
    me = lax.axis_index("exp")
    width = tok.shape[2]
    hidden = wi.shape[2]
    rows = n * b
    padded = n * pad

    loads = {}
    pairs = [
        ("log", log_hbm, logv), ("og", og_hbm, og), ("so", so_hbm, so), ("si", si_hbm, si),
        ("wi", wi_hbm, wi), ("bi", bi_hbm, bi), ("wo", wo_hbm, wo), ("tok", tok_hbm, tok), ("rt", rt_hbm, rt),
    ]
    for at, (name, src, dst) in enumerate(pairs):
        loads[name] = pltpu.make_async_copy(src, dst, load_sem.at[at])
        loads[name].start()

    barrier = pltpu.get_barrier_semaphore()

    def greet(d, _):
        peer = lax.rem(me + d, n)
        pl.semaphore_signal(barrier, inc=1, device_id={"exp": peer}, device_id_type=MESH)
        return 0

    lax.fori_loop(1, n, greet, 0)

    def remote(src, dst, send_sem, recv_sem, peer, slot):
        return pltpu.make_async_remote_copy(
            src_ref=src.at[peer], dst_ref=dst.at[slot], send_sem=send_sem.at[peer],
            recv_sem=recv_sem.at[slot], device_id={"exp": peer}, device_id_type=MESH,
        )

    def send_all(src, dst, send_sem, recv_sem):
        def step(d, _):
            remote(src, dst, send_sem, recv_sem, lax.rem(me + d, n), me).start()
            return 0

        lax.fori_loop(1, n, step, 0)
        dst[me] = src[me]

    def wait_all(src, dst, send_sem, recv_sem):
        def step(d, _):
            peer = lax.rem(me + n - d, n)
            remote(src, dst, send_sem, recv_sem, peer, peer).wait_recv()
            return 0

        lax.fori_loop(1, n, step, 0)

    def drain(src, dst, send_sem, recv_sem):
        def step(d, _):
            remote(src, dst, send_sem, recv_sem, lax.rem(me + d, n), me).wait_send()
            return 0

        lax.fori_loop(1, n, step, 0)

    spread = ones_where(padded, rows, lambda r, c: (r % pad < b) & (c == (r // pad) * b + r % pad))
    to_peers = ones_where(padded, rows, lambda r, c: (r % pad < b) & (c == (r % pad) * n + r // pad))
    to_images = ones_where(rows, padded, lambda r, c: c == (r % n) * pad + r // n)

    def grouped(x):
        return x.reshape(n, pad, width).astype(BF16)

    def flat(x):
        return x.astype(F32).reshape(padded, width).astype(BF16)

    loads["so"].wait()
    send_s[...] = grouped(dot(spread, so[0]))
    pl.semaphore_wait(barrier, n - 1)
    send_all(send_s, recv_s, ss, rs)

    loads["log"].wait()
    loads["og"].wait()
    for i in range(b):
        lt = logv[i].T
        e = jnp.exp(lt - jnp.max(lt, axis=0, keepdims=True))
        c = e / jnp.sum(e, axis=0, keepdims=True)
        comb[i] = c
        sg[i * n:(i + 1) * n, :] = dot(c.astype(BF16), og[i]).astype(BF16)
    send_a[...] = grouped(dot(to_peers, sg[...]))
    send_all(send_a, recv_a, sa, ra)

    for i in range(b):
        lt = logv[i].T
        e = jnp.exp(lt - jnp.max(lt, axis=1, keepdims=True))
        disp[i] = e / jnp.sum(e, axis=1, keepdims=True)

    loads["si"].wait()
    sip[...] = dot(spread, si[0]).astype(BF16)
    loads["wi"].wait()
    loads["bi"].wait()
    for k in range(0, hidden, chunk):
        hp = dot(sip[...], wi[0, :, k:k + chunk]) + bi[:, k:k + chunk]
        slope[:, k:k + chunk] = gelu_slope(hp)

    loads["wo"].wait()
    wait_all(send_a, recv_a, sa, ra)
    got = flat(recv_a[...])
    acc = jnp.zeros((padded, width), F32)
    for k in range(0, hidden, chunk):
        hg = dot_nt(got, wo[0, k:k + chunk, :])
        pre = (hg * slope[:, k:k + chunk]).astype(BF16)
        acc = acc + dot_nt(pre, wi[0, :, k:k + chunk])
    send_b[...] = grouped(acc)
    send_all(send_b, recv_b, sb, rb)

    loads["tok"].wait()
    loads["rt"].wait()
    wait_all(send_s, recv_s, ss, rs)
    outs = dot(to_images, flat(recv_s[...])).astype(BF16)
    racc = jnp.zeros((n, width), F32)
    for i in range(b):
        cg = dot_nt(outs[i * n:(i + 1) * n, :], og[i])
        c = comb[i]
        cl = (c * (cg - jnp.sum(c * cg, axis=0, keepdims=True))).astype(BF16)
        combl[i] = cl
        racc = racc + dot(cl, tok[i])

    wait_all(send_b, recv_b, sb, rb)
    sg[...] = dot(to_images, flat(recv_b[...])).astype(BF16)
    for i in range(b):
        dg = dot_nt(sg[i * n:(i + 1) * n, :], tok[i])
        d = disp[i]
        dl = (d * (dg - jnp.sum(d * dg, axis=1, keepdims=True))).astype(BF16)
        displ[i] = dl
        racc = racc + dot(dl, tok[i])
    send_r[...] = racc.reshape(n, 1, width)
    send_all(send_r, recv_r, sr, rr)

    outs_dma = []
    for i in range(b):
        left = jnp.concatenate([disp[i].astype(BF16), combl[i], displ[i]], axis=0)
        right = jnp.concatenate([sg[i * n:(i + 1) * n, :], rt[...], rt[...]], axis=0)
        igv[i] = dot_tn(left, right).astype(BF16)
        copy = pltpu.make_async_copy(igv.at[i], ig_hbm.at[i], out_sem.at[i])
        copy.start()
        outs_dma.append(copy)

    wait_all(send_r, recv_r, sr, rr)
    rg_ref[...] = jnp.sum(recv_r[...], axis=0) / (n * b)
    drain(send_s, recv_s, ss, rs)
    drain(send_a, recv_a, sa, ra)
    drain(send_b, recv_b, sb, rb)
    drain(send_r, recv_r, sr, rr)
    for copy in outs_dma:
        copy.wait()


def on_device(tokens, logits, slot_out, slot_in, out_grad, router, w_in, bias_in, w_out):
    b, seq, width = tokens.shape
    n = lax.axis_size("exp")
    hidden = w_in.shape[2]
    pad = -(-b // 8) * 8
    padded = n * pad
    chunk = 768 if hidden % 768 == 0 else hidden
    any_spec = pl.BlockSpec(memory_space=pl.ANY)
    exchange = pltpu.VMEM((n, pad, width), BF16)
    small = pltpu.VMEM((n, 1, width), F32)
    sems = pltpu.SemaphoreType.DMA((n,))
    return pl.pallas_call(
        functools.partial(body, n, b, pad, chunk),
        out_shape=(
            jax.ShapeDtypeStruct((b, seq, width), BF16),
            jax.ShapeDtypeStruct((1, width), F32),
        ),
        in_specs=[any_spec] * 9,
        out_specs=(any_spec, pl.BlockSpec(memory_space=pltpu.VMEM)),
        scratch_shapes=[
            pltpu.VMEM(tokens.shape, BF16),
            pltpu.VMEM(logits.shape, F32),
            pltpu.VMEM(slot_out.shape, BF16),
            pltpu.VMEM(slot_in.shape, BF16),
            pltpu.VMEM(out_grad.shape, BF16),
            pltpu.VMEM(router.shape, BF16),
            pltpu.VMEM(w_in.shape, BF16),
            pltpu.VMEM(bias_in.shape, F32),
            pltpu.VMEM(w_out.shape, BF16),
            pltpu.VMEM((b, seq, width), BF16),
            pltpu.VMEM((b, n, seq), F32),
            pltpu.VMEM((b, n, seq), F32),
            pltpu.VMEM((b, n, seq), BF16),
            pltpu.VMEM((b, n, seq), BF16),
            pltpu.VMEM((padded, hidden), F32),
            pltpu.VMEM((n * b, width), BF16),
            pltpu.VMEM((padded, width), BF16),
            exchange, exchange, exchange, exchange, exchange, exchange, small, small,
            pltpu.SemaphoreType.DMA((9,)),
            pltpu.SemaphoreType.DMA((b,)),
            sems, sems, sems, sems, sems, sems, sems, sems,
        ],
        compiler_params=pltpu.CompilerParams(
            collective_id=0, has_side_effects=True, vmem_limit_bytes=60 * 1024 * 1024
        ),
        name="moe_input_grad",
    )(tokens, logits, slot_out, slot_in, out_grad, router, w_in, bias_in, w_out)


def solution(mesh):
    placed = (
        P(("grp", "exp"), None, None),
        P(("grp", "exp"), None, None),
        P(("grp", "exp"), None, None),
        P(("grp", "exp"), None, None),
        P(("grp", "exp"), None, None),
        P(),
        P("exp", None, None),
        P("exp", None),
        P("exp", None, None),
    )
    return jax.shard_map(
        on_device,
        mesh=mesh,
        in_specs=placed,
        out_specs=(P(("grp", "exp"), None, None), P(("grp", "exp"), None)),
        check_vma=False,
    )
```

```python
import functools

import jax
import jax.numpy as jnp
from jax import lax
from jax.experimental import pallas as pl
from jax.experimental.pallas import tpu as pltpu
from jax.sharding import PartitionSpec as P

gelu_root = 0.7978845608028654
gelu_cubic = 0.044715
MESH = pl.DeviceIdType.MESH
F32 = jnp.float32
BF16 = jnp.bfloat16


def gelu_slope(values):
    square = values * values
    inner_arg = gelu_root * (values + gelu_cubic * square * values)
    tanh_val = jnp.tanh(inner_arg)
    return 0.5 * (1.0 + tanh_val) + 0.5 * values * (1.0 - tanh_val * tanh_val) * gelu_root * (
        1.0 + 3.0 * gelu_cubic * square
    )


def dot(a, b):
    return lax.dot_general(a, b, (((1,), (0,)), ((), ())), preferred_element_type=F32)


def dot_nt(a, b):
    return lax.dot_general(a, b, (((1,), (1,)), ((), ())), preferred_element_type=F32)


def dot_tn(a, b):
    return lax.dot_general(a, b, (((0,), (0,)), ((), ())), preferred_element_type=F32)


def ones_where(rows, cols, wanted):
    r = lax.broadcasted_iota(jnp.int32, (rows, cols), 0)
    c = lax.broadcasted_iota(jnp.int32, (rows, cols), 1)
    return jnp.where(wanted(r, c), 1.0, 0.0).astype(BF16)


def body(
    n, b, pad, chunk,
    tok_hbm, log_hbm, so_hbm, si_hbm, og_hbm, rt_hbm, wi_hbm, bi_hbm, wo_hbm,
    ig_hbm, rg_ref,
    tok, logv, so, si, og, rt, wi, bi, wo, igv,
    comb, disp, combl, displ, slope, sg, sip,
    send_s, recv_s, send_a, recv_a, send_b, recv_b, send_r, recv_r,
    load_sem, out_sem, ss, rs, sa, ra, sb, rb, sr, rr,
):
    me = lax.axis_index("exp")
    width = tok.shape[2]
    hidden = wi.shape[2]
    rows = n * b
    padded = n * pad

    loads = {}
    pairs = [
        ("log", log_hbm, logv), ("og", og_hbm, og), ("so", so_hbm, so), ("si", si_hbm, si),
        ("wi", wi_hbm, wi), ("bi", bi_hbm, bi), ("wo", wo_hbm, wo), ("tok", tok_hbm, tok), ("rt", rt_hbm, rt),
    ]
    for at, (name, src, dst) in enumerate(pairs):
        loads[name] = pltpu.make_async_copy(src, dst, load_sem.at[at])
        loads[name].start()

    if pad != b:
        for ref in (recv_s, recv_a, recv_b):
            ref[...] = jnp.zeros_like(ref)

    barrier = pltpu.get_barrier_semaphore()

    def greet(d, _):
        peer = lax.rem(me + d, n)
        pl.semaphore_signal(barrier, inc=1, device_id={"exp": peer}, device_id_type=MESH)
        return 0

    lax.fori_loop(1, n, greet, 0)

    def remote(src, dst, send_sem, recv_sem, peer, slot):
        return pltpu.make_async_remote_copy(
            src_ref=src.at[peer, :b], dst_ref=dst.at[slot, :b], send_sem=send_sem.at[peer],
            recv_sem=recv_sem.at[slot], device_id={"exp": peer}, device_id_type=MESH,
        )

    def send_all(src, dst, send_sem, recv_sem):
        def step(d, _):
            remote(src, dst, send_sem, recv_sem, lax.rem(me + d, n), me).start()
            return 0

        lax.fori_loop(1, n, step, 0)
        dst[me] = src[me]

    def wait_all(src, dst, send_sem, recv_sem):
        def step(d, _):
            peer = lax.rem(me + n - d, n)
            remote(src, dst, send_sem, recv_sem, peer, peer).wait_recv()
            return 0

        lax.fori_loop(1, n, step, 0)

    def drain(src, dst, send_sem, recv_sem):
        def step(d, _):
            remote(src, dst, send_sem, recv_sem, lax.rem(me + d, n), me).wait_send()
            return 0

        lax.fori_loop(1, n, step, 0)

    spread = ones_where(padded, rows, lambda r, c: (r % pad < b) & (c == (r // pad) * b + r % pad))
    to_peers = ones_where(padded, rows, lambda r, c: (r % pad < b) & (c == (r % pad) * n + r // pad))
    to_images = ones_where(rows, padded, lambda r, c: c == (r % n) * pad + r // n)

    def grouped(x):
        return x.reshape(n, pad, width).astype(BF16)

    def flat(x):
        return x.astype(F32).reshape(padded, width).astype(BF16)

    loads["log"].wait()
    loads["og"].wait()
    for i in range(b):
        lt = logv[i]
        e = jnp.exp(lt - jnp.max(lt, axis=0, keepdims=True))
        c = e / jnp.sum(e, axis=0, keepdims=True)
        comb[i] = c
        sg[i * n:(i + 1) * n, :] = dot(c.astype(BF16), og[i]).astype(BF16)
    send_a[...] = grouped(dot(to_peers, sg[...]))
    pl.semaphore_wait(barrier, n - 1)
    send_all(send_a, recv_a, sa, ra)
    loads["so"].wait()
    send_s[...] = grouped(dot(spread, so[0]))
    send_all(send_s, recv_s, ss, rs)

    for i in range(b):
        lt = logv[i]
        e = jnp.exp(lt - jnp.max(lt, axis=1, keepdims=True))
        disp[i] = e / jnp.sum(e, axis=1, keepdims=True)

    loads["si"].wait()
    sip[...] = dot(spread, si[0]).astype(BF16)
    loads["wi"].wait()
    loads["bi"].wait()
    for k in range(0, hidden, chunk):
        hp = dot(sip[...], wi[0, :, k:k + chunk]) + bi[:, k:k + chunk]
        slope[:, k:k + chunk] = gelu_slope(hp)

    loads["wo"].wait()
    wait_all(send_a, recv_a, sa, ra)
    got = flat(recv_a[...])
    acc = jnp.zeros((padded, width), F32)
    for k in range(0, hidden, chunk):
        hg = dot_nt(got, wo[0, k:k + chunk, :])
        pre = (hg * slope[:, k:k + chunk]).astype(BF16)
        acc = acc + dot_nt(pre, wi[0, :, k:k + chunk])
    send_b[...] = grouped(acc)
    send_all(send_b, recv_b, sb, rb)

    loads["tok"].wait()
    loads["rt"].wait()
    wait_all(send_s, recv_s, ss, rs)
    outs = dot(to_images, flat(recv_s[...])).astype(BF16)
    racc = jnp.zeros((n, width), F32)
    for i in range(b):
        cg = dot_nt(outs[i * n:(i + 1) * n, :], og[i])
        c = comb[i]
        cl = (c * (cg - jnp.sum(c * cg, axis=0, keepdims=True))).astype(BF16)
        combl[i] = cl
        racc = racc + dot(cl, tok[i])

    wait_all(send_b, recv_b, sb, rb)
    sg[...] = dot(to_images, flat(recv_b[...])).astype(BF16)
    for i in range(b):
        dg = dot_nt(sg[i * n:(i + 1) * n, :], tok[i])
        d = disp[i]
        dl = (d * (dg - jnp.sum(d * dg, axis=1, keepdims=True))).astype(BF16)
        displ[i] = dl
        racc = racc + dot(dl, tok[i])
    send_r[...] = racc.reshape(n, 1, width)
    send_all(send_r, recv_r, sr, rr)

    outs_dma = []
    for i in range(b):
        left = jnp.concatenate([disp[i].astype(BF16), combl[i], displ[i]], axis=0)
        right = jnp.concatenate([sg[i * n:(i + 1) * n, :], rt[...], rt[...]], axis=0)
        igv[i] = dot_tn(left, right).astype(BF16)
        copy = pltpu.make_async_copy(igv.at[i], ig_hbm.at[i], out_sem.at[i])
        copy.start()
        outs_dma.append(copy)

    wait_all(send_r, recv_r, sr, rr)
    rg_ref[...] = jnp.sum(recv_r[...], axis=0) / (n * b)
    drain(send_s, recv_s, ss, rs)
    drain(send_a, recv_a, sa, ra)
    drain(send_b, recv_b, sb, rb)
    drain(send_r, recv_r, sr, rr)
    for copy in outs_dma:
        copy.wait()


def on_device(tokens, logits, slot_out, slot_in, out_grad, router, w_in, bias_in, w_out):
    b, seq, width = tokens.shape
    n = lax.axis_size("exp")
    hidden = w_in.shape[2]
    pad = -(-b // 8) * 8
    padded = n * pad
    chunk = 768 if hidden % 768 == 0 else hidden
    hbm_spec = pl.BlockSpec(memory_space=pltpu.HBM)
    any_spec = pl.BlockSpec(memory_space=pl.ANY)
    limit = 67043328 - 65536 - b * (-(-seq // 8) * 8) * width * 2
    exchange = pltpu.VMEM((n, pad, width), BF16)
    small = pltpu.VMEM((n, 1, width), F32)
    sems = pltpu.SemaphoreType.DMA((n,))
    return pl.pallas_call(
        functools.partial(body, n, b, pad, chunk),
        out_shape=(
            pltpu.VMEM((b, seq, width), BF16),
            pltpu.VMEM((1, width), F32),
        ),
        in_specs=[hbm_spec] * 9,
        out_specs=(any_spec, pl.BlockSpec(memory_space=pltpu.VMEM)),
        scratch_shapes=[
            pltpu.VMEM(tokens.shape, BF16),
            pltpu.VMEM((b, n, seq), F32),
            pltpu.VMEM(slot_out.shape, BF16),
            pltpu.VMEM(slot_in.shape, BF16),
            pltpu.VMEM(out_grad.shape, BF16),
            pltpu.VMEM(router.shape, BF16),
            pltpu.VMEM(w_in.shape, BF16),
            pltpu.VMEM(bias_in.shape, F32),
            pltpu.VMEM(w_out.shape, BF16),
            pltpu.VMEM((b, seq, width), BF16),
            pltpu.VMEM((b, n, seq), F32),
            pltpu.VMEM((b, n, seq), F32),
            pltpu.VMEM((b, n, seq), BF16),
            pltpu.VMEM((b, n, seq), BF16),
            pltpu.VMEM((padded, hidden), F32),
            pltpu.VMEM((n * b, width), BF16),
            pltpu.VMEM((padded, width), BF16),
            exchange, exchange, exchange, exchange, exchange, exchange, small, small,
            pltpu.SemaphoreType.DMA((9,)),
            pltpu.SemaphoreType.DMA((b,)),
            sems, sems, sems, sems, sems, sems, sems, sems,
        ],
        compiler_params=pltpu.CompilerParams(
            collective_id=0, has_side_effects=True, vmem_limit_bytes=limit
        ),
        name="moe_input_grad",
    )(tokens, jnp.swapaxes(logits, 1, 2), slot_out, slot_in, out_grad, router, w_in, bias_in, w_out)


def solution(mesh):
    placed = (
        P(("grp", "exp"), None, None),
        P(("grp", "exp"), None, None),
        P(("grp", "exp"), None, None),
        P(("grp", "exp"), None, None),
        P(("grp", "exp"), None, None),
        P(),
        P("exp", None, None),
        P("exp", None),
        P("exp", None, None),
    )
    return jax.shard_map(
        on_device,
        mesh=mesh,
        in_specs=placed,
        out_specs=(P(("grp", "exp"), None, None), P(("grp", "exp"), None)),
        check_vma=False,
    )
```

```python
import functools

import jax
import jax.numpy as jnp
from jax import lax
from jax.experimental import pallas as pl
from jax.experimental.pallas import tpu as pltpu
from jax.sharding import PartitionSpec as P

gelu_root = 0.7978845608028654
gelu_cubic = 0.044715
MESH = pl.DeviceIdType.MESH
F32 = jnp.float32
BF16 = jnp.bfloat16


def gelu_slope(values):
    square = values * values
    inner_arg = gelu_root * (values + gelu_cubic * square * values)
    tanh_val = jnp.tanh(inner_arg)
    return 0.5 * (1.0 + tanh_val) + 0.5 * values * (1.0 - tanh_val * tanh_val) * gelu_root * (
        1.0 + 3.0 * gelu_cubic * square
    )


def dot(a, b):
    return lax.dot_general(a, b, (((1,), (0,)), ((), ())), preferred_element_type=F32)


def dot_nt(a, b):
    return lax.dot_general(a, b, (((1,), (1,)), ((), ())), preferred_element_type=F32)


def dot_tn(a, b):
    return lax.dot_general(a, b, (((0,), (0,)), ((), ())), preferred_element_type=F32)


def ones_where(rows, cols, wanted):
    r = lax.broadcasted_iota(jnp.int32, (rows, cols), 0)
    c = lax.broadcasted_iota(jnp.int32, (rows, cols), 1)
    return jnp.where(wanted(r, c), 1.0, 0.0).astype(BF16)


def body(
    n, b, pad, chunk,
    tok_hbm, log_hbm, so_hbm, si_hbm, og_hbm, rt_hbm, wi_hbm, bi_hbm, wo_hbm,
    ig_ref, rg_ref,
    tok, logv, so, si, og, rt, wi, bi, wo,
    comb, disp, combl, displ, slope, sg, sip,
    send_s, recv_s, send_a, recv_a, send_b, recv_b, send_r, recv_r, tok_t, pre, wi_t,
    load_sem, sem_a, sem_s, sem_b, sem_r,
):
    me = lax.axis_index("exp")
    width = tok.shape[2]
    hidden = wi.shape[2]
    rows = n * b
    padded = n * pad

    loads = {}
    pairs = [
        ("log", log_hbm, logv), ("og", og_hbm, og), ("so", so_hbm, so), ("si", si_hbm, si),
        ("wi", wi_hbm, wi), ("bi", bi_hbm, bi), ("wo", wo_hbm, wo), ("tok", tok_hbm, tok), ("rt", rt_hbm, rt),
    ]
    for at, (name, src, dst) in enumerate(pairs):
        loads[name] = pltpu.make_async_copy(src, dst, load_sem.at[at])
        loads[name].start()

    if pad != b:
        for ref in (recv_s, recv_a, recv_b):
            ref[...] = jnp.zeros_like(ref)

    barrier = pltpu.get_barrier_semaphore()

    def greet(d, _):
        peer = lax.rem(me + d, n)
        pl.semaphore_signal(barrier, inc=1, device_id={"exp": peer}, device_id_type=MESH)
        return 0

    lax.fori_loop(1, n, greet, 0)

    def remote(src, dst, sems, peer):
        return pltpu.make_async_remote_copy(
            src_ref=src.at[peer, :rows_of(src)], dst_ref=dst.at[me, :rows_of(src)], send_sem=sems.at[0],
            recv_sem=sems.at[1], device_id={"exp": peer}, device_id_type=MESH,
        )

    def rows_of(ref):
        return min(b, ref.shape[1])

    def send_all(src, dst, sems):
        def step(k, _):
            away = n // 2 + (k // 2) * (1 - 2 * (k % 2))
            remote(src, dst, sems, lax.rem(me + away, n)).start()
            return 0

        lax.fori_loop(1, n, step, 0)
        dst[me] = src[me]

    def everything(src, dst, sems):
        return pltpu.make_async_remote_copy(
            src_ref=src.at[:n - 1, :rows_of(src)], dst_ref=dst.at[:n - 1, :rows_of(src)], send_sem=sems.at[0],
            recv_sem=sems.at[1], device_id={"exp": lax.rem(me + 1, n)}, device_id_type=MESH,
        )

    def wait_all(src, dst, sems):
        everything(src, dst, sems).wait_recv()

    def drain(src, dst, sems):
        everything(src, dst, sems).wait_send()

    spread = ones_where(padded, rows, lambda r, c: (r % pad < b) & (c == (r // pad) * b + r % pad))
    to_peers = ones_where(padded, rows, lambda r, c: (r % pad < b) & (c == (r % pad) * n + r // pad))
    to_images = ones_where(rows, padded, lambda r, c: c == (r % n) * pad + r // n)

    def grouped(x):
        return x.reshape(n, pad, x.shape[1]).astype(BF16)

    def flat(x):
        return x.astype(F32).reshape(padded, x.shape[2]).astype(BF16)

    loads["log"].wait()
    loads["og"].wait()
    for i in range(b):
        lt = logv[i]
        e = jnp.exp(lt - jnp.max(lt, axis=0, keepdims=True))
        c = e / jnp.sum(e, axis=0, keepdims=True)
        comb[i] = c
        sg[i * n:(i + 1) * n, :] = dot(c.astype(BF16), og[i]).astype(BF16)
    send_a[...] = grouped(dot(to_peers, sg[...]))
    pl.semaphore_wait(barrier, n - 1)
    send_all(send_a, recv_a, sem_a)
    loads["so"].wait()
    send_s[...] = grouped(dot(spread, so[0]))
    send_all(send_s, recv_s, sem_s)

    for i in range(b):
        lt = logv[i]
        e = jnp.exp(lt - jnp.max(lt, axis=1, keepdims=True))
        disp[i] = e / jnp.sum(e, axis=1, keepdims=True)

    loads["si"].wait()
    sip[...] = dot(spread, si[0]).astype(BF16)
    loads["wi"].wait()
    loads["bi"].wait()
    for k in range(0, hidden, chunk):
        hp = dot(sip[...], wi[0, :, k:k + chunk]) + bi[:, k:k + chunk]
        slope[:, k:k + chunk] = gelu_slope(hp)
        wi_t[k:k + chunk, :] = wi[0, :, k:k + chunk].T

    loads["wo"].wait()
    wait_all(send_a, recv_a, sem_a)
    got = flat(recv_a[...])
    for k in range(0, hidden, chunk):
        hg = dot_nt(got, wo[0, k:k + chunk, :])
        pre[:, k:k + chunk] = (hg * slope[:, k:k + chunk]).astype(BF16)
    blocks, block = send_b.shape[0], send_b.shape[3]
    for q in range(blocks):
        acc = dot(pre[...], wi_t[:, q * block:(q + 1) * block])
        send_b[q] = grouped(acc)
        send_all(send_b.at[q], recv_b.at[q], sem_b.at[q])

    loads["tok"].wait()
    loads["rt"].wait()
    wait_all(send_s, recv_s, sem_s)
    outs = dot(to_images, flat(recv_s[...])).astype(BF16)
    racc = jnp.zeros((n, width), F32)
    for i in range(b):
        cg = dot_nt(outs[i * n:(i + 1) * n, :], og[i])
        c = comb[i]
        cl = (c * (cg - jnp.sum(c * cg, axis=0, keepdims=True))).astype(BF16)
        combl[i] = cl
        racc = racc + dot(cl, tok[i])
        tok_t[i] = tok[i].T

    for q in range(blocks):
        wait_all(send_b.at[q], recv_b.at[q], sem_b.at[q])
        sg[:, q * block:(q + 1) * block] = dot(to_images, flat(recv_b[q])).astype(BF16)
    for i in range(b):
        dg = dot(sg[i * n:(i + 1) * n, :], tok_t[i])
        d = disp[i]
        dl = (d * (dg - jnp.sum(d * dg, axis=1, keepdims=True))).astype(BF16)
        displ[i] = dl
        racc = racc + dot(dl, tok[i])
    send_r[...] = racc.reshape(n, 1, width)
    send_all(send_r, recv_r, sem_r)

    for i in range(b):
        left = jnp.concatenate([disp[i].astype(BF16), combl[i], displ[i]], axis=0)
        right = jnp.concatenate([sg[i * n:(i + 1) * n, :], rt[...], rt[...]], axis=0)
        ig_ref[i] = dot_tn(left, right).astype(BF16)

    drain(send_s, recv_s, sem_s)
    drain(send_a, recv_a, sem_a)
    for q in range(blocks):
        drain(send_b.at[q], recv_b.at[q], sem_b.at[q])
    wait_all(send_r, recv_r, sem_r)
    rg_ref[...] = jnp.sum(recv_r[...], axis=0) / (n * b)
    drain(send_r, recv_r, sem_r)


def on_device(tokens, logits, slot_out, slot_in, out_grad, router, w_in, bias_in, w_out):
    b, seq, width = tokens.shape
    n = lax.axis_size("exp")
    hidden = w_in.shape[2]
    pad = -(-b // 8) * 8
    padded = n * pad
    chunk = 768 if hidden % 768 == 0 else hidden
    hbm_spec = pl.BlockSpec(memory_space=pltpu.HBM)
    limit = 67043328 - 65536 - b * (-(-seq // 8) * 8) * width * 2
    exchange = pltpu.VMEM((n, pad, width), BF16)
    small = pltpu.VMEM((n, 1, width), F32)
    sems = pltpu.SemaphoreType.DMA((2,))
    block = 256 if width % 256 == 0 else width
    columns = pltpu.VMEM((width // block, n, pad, block), BF16)
    return pl.pallas_call(
        functools.partial(body, n, b, pad, chunk),
        out_shape=(
            pltpu.VMEM((b, seq, width), BF16),
            pltpu.VMEM((1, width), F32),
        ),
        in_specs=[hbm_spec] * 9,
        out_specs=(pl.BlockSpec(memory_space=pltpu.VMEM), pl.BlockSpec(memory_space=pltpu.VMEM)),
        scratch_shapes=[
            pltpu.VMEM(tokens.shape, BF16),
            pltpu.VMEM((b, n, seq), F32),
            pltpu.VMEM(slot_out.shape, BF16),
            pltpu.VMEM(slot_in.shape, BF16),
            pltpu.VMEM(out_grad.shape, BF16),
            pltpu.VMEM(router.shape, BF16),
            pltpu.VMEM(w_in.shape, BF16),
            pltpu.VMEM(bias_in.shape, F32),
            pltpu.VMEM(w_out.shape, BF16),
            pltpu.VMEM((b, n, seq), F32),
            pltpu.VMEM((b, n, seq), F32),
            pltpu.VMEM((b, n, seq), BF16),
            pltpu.VMEM((b, n, seq), BF16),
            pltpu.VMEM((padded, hidden), F32),
            pltpu.VMEM((n * b, width), BF16),
            pltpu.VMEM((padded, width), BF16),
            exchange, exchange, exchange, exchange, columns, columns, small, small,
            pltpu.VMEM((b, width, seq), BF16),
            pltpu.VMEM((padded, hidden), BF16),
            pltpu.VMEM((hidden, width), BF16),
            pltpu.SemaphoreType.DMA((9,)),
            sems, sems, pltpu.SemaphoreType.DMA((width // block, 2)), sems,
        ],
        compiler_params=pltpu.CompilerParams(
            collective_id=0, has_side_effects=True, vmem_limit_bytes=limit
        ),
        name="moe_input_grad",
    )(tokens, jnp.swapaxes(logits, 1, 2), slot_out, slot_in, out_grad, router, w_in, bias_in, w_out)


def solution(mesh):
    placed = (
        P(("grp", "exp"), None, None),
        P(("grp", "exp"), None, None),
        P(("grp", "exp"), None, None),
        P(("grp", "exp"), None, None),
        P(("grp", "exp"), None, None),
        P(),
        P("exp", None, None),
        P("exp", None),
        P("exp", None, None),
    )
    return jax.shard_map(
        on_device,
        mesh=mesh,
        in_specs=placed,
        out_specs=(P(("grp", "exp"), None, None), P(("grp", "exp"), None)),
        check_vma=False,
    )
```

```python
import functools

import jax
import jax.numpy as jnp
from jax import lax
from jax.experimental import pallas as pl
from jax.experimental.pallas import tpu as pltpu
from jax.sharding import PartitionSpec as P

gelu_root = 0.7978845608028654
gelu_cubic = 0.044715
MESH = pl.DeviceIdType.MESH
F32 = jnp.float32
BF16 = jnp.bfloat16


def gelu_slope(values):
    square = values * values
    inner_arg = gelu_root * (values + gelu_cubic * square * values)
    tanh_val = jnp.tanh(inner_arg)
    return 0.5 * (1.0 + tanh_val) + 0.5 * values * (1.0 - tanh_val * tanh_val) * gelu_root * (
        1.0 + 3.0 * gelu_cubic * square
    )


def dot(a, b):
    return lax.dot_general(a, b, (((1,), (0,)), ((), ())), preferred_element_type=F32)


def dot_nt(a, b):
    return lax.dot_general(a, b, (((1,), (1,)), ((), ())), preferred_element_type=F32)


def dot_tn(a, b):
    return lax.dot_general(a, b, (((0,), (0,)), ((), ())), preferred_element_type=F32)


def ones_where(rows, cols, wanted):
    r = lax.broadcasted_iota(jnp.int32, (rows, cols), 0)
    c = lax.broadcasted_iota(jnp.int32, (rows, cols), 1)
    return jnp.where(wanted(r, c), 1.0, 0.0).astype(BF16)


def body(
    n, b, pad, chunk,
    tok_hbm, log_hbm, so_hbm, si_hbm, og_hbm, rt_hbm, wi_hbm, bi_hbm, wo_hbm,
    ig_ref, rg_ref,
    tok, logv, so, si, og, rt, wi, bi, wo,
    comb, disp, combl, displ, slope, sg, sip,
    send_s, recv_s, send_a, recv_a, send_b, recv_b, send_r, recv_r, tok_t, pre, wi_t,
    load_sem, sem_a, sem_s, sem_b, sem_r,
):
    me = lax.axis_index("exp")
    width = tok.shape[2]
    hidden = wi.shape[2]
    rows = n * b
    padded = n * pad

    loads = {}
    pairs = [
        ("log", log_hbm, logv), ("og", og_hbm, og), ("so", so_hbm, so), ("si", si_hbm, si),
        ("wi", wi_hbm, wi), ("bi", bi_hbm, bi), ("wo", wo_hbm, wo), ("tok", tok_hbm, tok), ("rt", rt_hbm, rt),
    ]
    for at, (name, src, dst) in enumerate(pairs):
        loads[name] = pltpu.make_async_copy(src, dst, load_sem.at[at])
        loads[name].start()

    if pad != b:
        for ref in (recv_s, recv_a, recv_b):
            ref[...] = jnp.zeros_like(ref)

    barrier = pltpu.get_barrier_semaphore()

    def greet(d, _):
        peer = lax.rem(me + d, n)
        pl.semaphore_signal(barrier, inc=1, device_id={"exp": peer}, device_id_type=MESH)
        return 0

    lax.fori_loop(1, n, greet, 0, unroll=True)

    def remote(src, dst, sems, peer):
        return pltpu.make_async_remote_copy(
            src_ref=src.at[peer, :rows_of(src)], dst_ref=dst.at[me, :rows_of(src)], send_sem=sems.at[0],
            recv_sem=sems.at[1], device_id={"exp": peer}, device_id_type=MESH,
        )

    def rows_of(ref):
        return min(b, ref.shape[1])

    def send_all(src, dst, sems):
        def step(k, _):
            away = n // 2 + (k // 2) * (1 - 2 * (k % 2))
            remote(src, dst, sems, lax.rem(me + away, n)).start()
            return 0

        lax.fori_loop(1, n, step, 0, unroll=True)
        dst[me] = src[me]

    def everything(src, dst, sems):
        return pltpu.make_async_remote_copy(
            src_ref=src.at[:n - 1, :rows_of(src)], dst_ref=dst.at[:n - 1, :rows_of(src)], send_sem=sems.at[0],
            recv_sem=sems.at[1], device_id={"exp": lax.rem(me + 1, n)}, device_id_type=MESH,
        )

    def wait_all(src, dst, sems):
        everything(src, dst, sems).wait_recv()

    def drain(src, dst, sems):
        everything(src, dst, sems).wait_send()

    spread = ones_where(padded, rows, lambda r, c: (r % pad < b) & (c == (r // pad) * b + r % pad))
    to_peers = ones_where(padded, rows, lambda r, c: (r % pad < b) & (c == (r % pad) * n + r // pad))
    to_images = ones_where(rows, padded, lambda r, c: c == (r % n) * pad + r // n)

    def grouped(x):
        return x.reshape(n, pad, x.shape[1]).astype(BF16)

    def flat(x):
        return x.astype(F32).reshape(padded, x.shape[2]).astype(BF16)

    loads["log"].wait()
    loads["og"].wait()
    for i in range(b):
        lt = logv[i]
        e = jnp.exp(lt - jnp.max(lt, axis=0, keepdims=True))
        c = e / jnp.sum(e, axis=0, keepdims=True)
        comb[i] = c
        sg[i * n:(i + 1) * n, :] = dot(c.astype(BF16), og[i]).astype(BF16)
    send_a[...] = grouped(dot(to_peers, sg[...]))
    pl.semaphore_wait(barrier, n - 1)
    send_all(send_a, recv_a, sem_a)
    loads["so"].wait()
    send_s[...] = grouped(dot(spread, so[0]))
    send_all(send_s, recv_s, sem_s)

    for i in range(b):
        lt = logv[i]
        e = jnp.exp(lt - jnp.max(lt, axis=1, keepdims=True))
        disp[i] = e / jnp.sum(e, axis=1, keepdims=True)

    loads["si"].wait()
    sip[...] = dot(spread, si[0]).astype(BF16)
    loads["wi"].wait()
    loads["bi"].wait()
    for k in range(0, hidden, chunk):
        hp = dot(sip[...], wi[0, :, k:k + chunk]) + bi[:, k:k + chunk]
        slope[:, k:k + chunk] = gelu_slope(hp)
        wi_t[k:k + chunk, :] = wi[0, :, k:k + chunk].T

    loads["wo"].wait()
    wait_all(send_a, recv_a, sem_a)
    got = flat(recv_a[...])
    for k in range(0, hidden, chunk):
        hg = dot_nt(got, wo[0, k:k + chunk, :])
        pre[:, k:k + chunk] = (hg * slope[:, k:k + chunk]).astype(BF16)
    blocks, block = send_b.shape[0], send_b.shape[3]
    for q in range(blocks):
        acc = dot(pre[...], wi_t[:, q * block:(q + 1) * block])
        send_b[q] = grouped(acc)
        send_all(send_b.at[q], recv_b.at[q], sem_b.at[q])

    loads["tok"].wait()
    loads["rt"].wait()
    wait_all(send_s, recv_s, sem_s)
    outs = dot(to_images, flat(recv_s[...])).astype(BF16)
    racc = jnp.zeros((n, width), F32)
    for i in range(b):
        cg = dot_nt(outs[i * n:(i + 1) * n, :], og[i])
        c = comb[i]
        cl = (c * (cg - jnp.sum(c * cg, axis=0, keepdims=True))).astype(BF16)
        combl[i] = cl
        racc = racc + dot(cl, tok[i])
        tok_t[i] = tok[i].T

    for q in range(blocks):
        wait_all(send_b.at[q], recv_b.at[q], sem_b.at[q])
        sg[:, q * block:(q + 1) * block] = dot(to_images, flat(recv_b[q])).astype(BF16)
    for i in range(b):
        dg = dot(sg[i * n:(i + 1) * n, :], tok_t[i])
        d = disp[i]
        dl = (d * (dg - jnp.sum(d * dg, axis=1, keepdims=True))).astype(BF16)
        displ[i] = dl
        racc = racc + dot(dl, tok[i])
    send_r[...] = racc.reshape(n, 1, width)
    send_all(send_r, recv_r, sem_r)

    for i in range(b):
        left = jnp.concatenate([disp[i].astype(BF16), combl[i], displ[i]], axis=0)
        right = jnp.concatenate([sg[i * n:(i + 1) * n, :], rt[...], rt[...]], axis=0)
        ig_ref[i] = dot_tn(left, right).astype(BF16)

    drain(send_s, recv_s, sem_s)
    drain(send_a, recv_a, sem_a)
    for q in range(blocks):
        drain(send_b.at[q], recv_b.at[q], sem_b.at[q])
    wait_all(send_r, recv_r, sem_r)
    rg_ref[...] = jnp.sum(recv_r[...], axis=0) / (n * b)
    drain(send_r, recv_r, sem_r)


def on_device(tokens, logits, slot_out, slot_in, out_grad, router, w_in, bias_in, w_out):
    b, seq, width = tokens.shape
    n = lax.axis_size("exp")
    hidden = w_in.shape[2]
    pad = -(-b // 8) * 8
    padded = n * pad
    chunk = 768 if hidden % 768 == 0 else hidden
    hbm_spec = pl.BlockSpec(memory_space=pltpu.HBM)
    limit = 67043328 - 65536 - b * (-(-seq // 8) * 8) * width * 2
    exchange = pltpu.VMEM((n, pad, width), BF16)
    small = pltpu.VMEM((n, 1, width), F32)
    sems = pltpu.SemaphoreType.DMA((2,))
    block = width // 2 if width % 256 == 0 else width
    columns = pltpu.VMEM((width // block, n, pad, block), BF16)
    return pl.pallas_call(
        functools.partial(body, n, b, pad, chunk),
        out_shape=(
            pltpu.VMEM((b, seq, width), BF16),
            pltpu.VMEM((1, width), F32),
        ),
        in_specs=[hbm_spec] * 9,
        out_specs=(pl.BlockSpec(memory_space=pltpu.VMEM), pl.BlockSpec(memory_space=pltpu.VMEM)),
        scratch_shapes=[
            pltpu.VMEM(tokens.shape, BF16),
            pltpu.VMEM((b, n, seq), F32),
            pltpu.VMEM(slot_out.shape, BF16),
            pltpu.VMEM(slot_in.shape, BF16),
            pltpu.VMEM(out_grad.shape, BF16),
            pltpu.VMEM(router.shape, BF16),
            pltpu.VMEM(w_in.shape, BF16),
            pltpu.VMEM(bias_in.shape, F32),
            pltpu.VMEM(w_out.shape, BF16),
            pltpu.VMEM((b, n, seq), F32),
            pltpu.VMEM((b, n, seq), F32),
            pltpu.VMEM((b, n, seq), BF16),
            pltpu.VMEM((b, n, seq), BF16),
            pltpu.VMEM((padded, hidden), F32),
            pltpu.VMEM((n * b, width), BF16),
            pltpu.VMEM((padded, width), BF16),
            exchange, exchange, exchange, exchange, columns, columns, small, small,
            pltpu.VMEM((b, width, seq), BF16),
            pltpu.VMEM((padded, hidden), BF16),
            pltpu.VMEM((hidden, width), BF16),
            pltpu.SemaphoreType.DMA((9,)),
            sems, sems, pltpu.SemaphoreType.DMA((width // block, 2)), sems,
        ],
        compiler_params=pltpu.CompilerParams(
            collective_id=0, has_side_effects=True, vmem_limit_bytes=limit
        ),
        name="moe_input_grad",
    )(tokens, jnp.swapaxes(logits, 1, 2), slot_out, slot_in, out_grad, router, w_in, bias_in, w_out)


def solution(mesh):
    placed = (
        P(("grp", "exp"), None, None),
        P(("grp", "exp"), None, None),
        P(("grp", "exp"), None, None),
        P(("grp", "exp"), None, None),
        P(("grp", "exp"), None, None),
        P(),
        P("exp", None, None),
        P("exp", None),
        P("exp", None, None),
    )
    return jax.shard_map(
        on_device,
        mesh=mesh,
        in_specs=placed,
        out_specs=(P(("grp", "exp"), None, None), P(("grp", "exp"), None)),
        check_vma=False,
    )
```
